32 devices in a mesh: fsdp: 4 (over z), ep: 8 (over y, x, core).
Axes of the slice: x: 2, y: 2, z: 4, core: 2. Of those that a mesh axis runs over, the one named last changes fastest.
Arguments:
- grad_out: bfloat16 [4096, 768], P(('fsdp', 'ep'))
- expert_idx: int32 [4096, 1], P(('fsdp', 'ep'))
- slot_pos: int32 [4096, 1], P(('fsdp', 'ep'))
- gates: float32 [4096, 1], P(('fsdp', 'ep'))
- x_disp: bfloat16 [32, 256, 768], P('ep', 'fsdp')
- h_gate: bfloat16 [32, 256, 3072], P('ep', 'fsdp')
- h_up: bfloat16 [32, 256, 3072], P('ep', 'fsdp')
- y_disp: bfloat16 [32, 256, 768], P('ep', 'fsdp')
- w_gate: bfloat16 [32, 768, 3072], P('ep', 'fsdp')
- w_down: bfloat16 [32, 3072, 768], P('ep', 'fsdp')
- w_up: bfloat16 [32, 768, 3072], P('ep', 'fsdp')
Outputs:
- output 1: bfloat16 [4096, 768], P(('fsdp', 'ep'))
- output 2: float32 [4096, 1], P(('fsdp', 'ep'))
- output 3: float32 [32, 768, 3072], P('ep', 'fsdp')
- output 4: float32 [32, 3072, 768], P('ep', 'fsdp')
- output 5: float32 [32, 768, 3072], P('ep', 'fsdp')
All inputs are finite; a program needn't handle non-finite values.
Results may differ from the reference program's by a relative error of at most 0.001.
Values are sent between devices in bfloat16 or wider.
A program may use at most 1 GiB of HBM per device.

```python
import jax
import jax.numpy as jnp
from jax import lax

D = 768
F = 3072
EXPERTS = 32
TOP = 1
TOK = 128
NDEV = 32
CAP = 8


def route_draw(key):
    key_bias, key_noise, key_hot = jax.random.split(key, 3)
    expert_ids = jnp.arange(EXPERTS, dtype=jnp.int32)
    expert_bias = jax.random.randint(key_bias, (EXPERTS,), 0, 512, dtype=jnp.int32)
    noise_int = jax.random.randint(key_noise, (NDEV, TOK, EXPERTS), 0, 1024, dtype=jnp.int32)
    hot_expert = jax.random.randint(key_hot, (NDEV,), 0, EXPERTS, dtype=jnp.int32)
    forced = (jnp.arange(TOK, dtype=jnp.int32)[None, :, None] <= CAP) & (expert_ids[None, None, :] == hot_expert[:, None, None])
    score_int = (noise_int + expert_bias + jnp.where(forced, 4096, 0)) * EXPERTS + expert_ids
    expert_idx = lax.top_k(score_int, TOP)[1].astype(jnp.int32)

    def block_slots(block_idx):
        flat_ids = block_idx.reshape(-1)
        hit_mask = (flat_ids[:, None] == expert_ids[None, :]).astype(jnp.int32)
        slot_rank = jnp.sum((jnp.cumsum(hit_mask, axis=0) - hit_mask) * hit_mask, axis=1)
        return jnp.where(slot_rank < CAP, slot_rank, -1).reshape(TOK, TOP)

    slot_pos = lax.map(block_slots, expert_idx)
    return expert_idx.reshape(NDEV * TOK, TOP), slot_pos.reshape(NDEV * TOK, TOP).astype(jnp.int32)


def setup_inputs(seed: int = 0) -> dict:
    keys = jax.random.split(jax.random.key(seed), 11)
    expert_idx, slot_pos = route_draw(keys[0])
    rows_all = NDEV * CAP
    grad_out = jax.random.normal(keys[1], (NDEV * TOK, D), jnp.float32).astype(jnp.bfloat16)
    gates = jax.random.uniform(keys[2], (NDEV * TOK, TOP), jnp.float32, 0.2, 1.0)
    x_disp = jax.random.normal(keys[3], (EXPERTS, rows_all, D), jnp.float32).astype(jnp.bfloat16)
    h_gate = jax.random.normal(keys[4], (EXPERTS, rows_all, F), jnp.float32).astype(jnp.bfloat16)
    h_up = jax.random.normal(keys[5], (EXPERTS, rows_all, F), jnp.float32).astype(jnp.bfloat16)
    y_disp = (0.25 * jax.random.normal(keys[6], (EXPERTS, rows_all, D), jnp.float32)).astype(jnp.bfloat16)
    w_gate = (jax.random.normal(keys[7], (EXPERTS, D, F), jnp.float32) * D ** -0.5).astype(jnp.bfloat16)
    w_down = (jax.random.normal(keys[8], (EXPERTS, F, D), jnp.float32) * F ** -0.5).astype(jnp.bfloat16)
    w_up = (jax.random.normal(keys[9], (EXPERTS, D, F), jnp.float32) * D ** -0.5).astype(jnp.bfloat16)
    return {'grad_out': grad_out, 'expert_idx': expert_idx, 'slot_pos': slot_pos, 'gates': gates, 'x_disp': x_disp, 'h_gate': h_gate, 'h_up': h_up, 'y_disp': y_disp, 'w_gate': w_gate, 'w_down': w_down, 'w_up': w_up}


def expert_backward(operands):
    dy_rows, gate_rows, x_rows, pre_gate, pre_up, y_rows, w_gate, w_down, w_up = operands
    g_rows = (dy_rows.astype(jnp.float32) * gate_rows[:, None]).astype(jnp.bfloat16)
    gate_pre = pre_gate.astype(jnp.float32)
    up_pre = pre_up.astype(jnp.float32)
    sigmoid_gate = jax.nn.sigmoid(gate_pre)
    silu_gate = gate_pre * sigmoid_gate
    act_rows = (silu_gate * up_pre).astype(jnp.bfloat16)
    d_act = jnp.dot(g_rows, w_down.T, preferred_element_type=jnp.float32)
    dh_gate = (d_act * up_pre * sigmoid_gate * (1.0 + gate_pre * (1.0 - sigmoid_gate))).astype(jnp.bfloat16)
    dh_up = (d_act * silu_gate).astype(jnp.bfloat16)
    dx_rows = (jnp.dot(dh_gate, w_gate.T, preferred_element_type=jnp.float32) + jnp.dot(dh_up, w_up.T, preferred_element_type=jnp.float32)).astype(jnp.bfloat16)
    dgate_rows = jnp.sum(dy_rows.astype(jnp.float32) * y_rows.astype(jnp.float32), axis=1)
    dw_gate = jnp.dot(x_rows.T, dh_gate, preferred_element_type=jnp.float32)
    dw_down = jnp.dot(act_rows.T, g_rows, preferred_element_type=jnp.float32)
    dw_up = jnp.dot(x_rows.T, dh_up, preferred_element_type=jnp.float32)
    return dx_rows, dgate_rows, dw_gate, dw_down, dw_up


def reference(grad_out, expert_idx, slot_pos, gates, x_disp, h_gate, h_up, y_disp, w_gate, w_down, w_up):
    rows_all = NDEV * CAP
    choices = NDEV * TOK * TOP
    block_ids = jnp.arange(NDEV * TOK, dtype=jnp.int32)[:, None] // TOK
    dest_row = jnp.where(slot_pos >= 0, expert_idx * rows_all + block_ids * CAP + slot_pos, EXPERTS * rows_all).reshape(-1)
    src_choice = jnp.full((EXPERTS * rows_all,), choices, jnp.int32).at[dest_row].set(jnp.arange(choices, dtype=jnp.int32), mode='drop')
    dy_rows = jnp.take(grad_out, src_choice // TOP, axis=0, mode='fill', fill_value=0).reshape(EXPERTS, rows_all, D)
    gate_rows = jnp.take(gates.reshape(-1), src_choice, mode='fill', fill_value=0).reshape(EXPERTS, rows_all)
    dx_rows, dgate_rows, dw_gate, dw_down, dw_up = lax.map(expert_backward, (dy_rows, gate_rows, x_disp, h_gate, h_up, y_disp, w_gate, w_down, w_up))
    picked = jnp.take(dx_rows.reshape(EXPERTS * rows_all, D), dest_row, axis=0, mode='fill', fill_value=0).reshape(NDEV * TOK, TOP, D)
    grad_x = jnp.sum(picked.astype(jnp.float32), axis=1).astype(jnp.bfloat16)
    grad_gates = jnp.take(dgate_rows.reshape(-1), dest_row, mode='fill', fill_value=0).reshape(NDEV * TOK, TOP)
    return grad_x, grad_gates, dw_gate, dw_down, dw_up
```

```python
import jax
import jax.numpy as jnp
from jax import lax
from jax.sharding import PartitionSpec as P


def solution(mesh):
    ep_n = mesh.shape['ep']
    fs_n = mesh.shape['fsdp']
    tok_spec = P(('fsdp', 'ep'), None)
    row_spec = P('ep', 'fsdp', None)

    def local_backward(grad_out, expert_idx, slot_pos, gates, x_disp, h_gate, h_up, y_disp, w_gate, w_down, w_up):
        tok_n, top_n = expert_idx.shape
        e_loc, rows_loc, width = x_disp.shape
        hidden = h_gate.shape[2]
        f_loc = hidden // fs_n
        d_loc = width // fs_n
        slot_cap = rows_loc // ep_n
        slots_n = e_loc * ep_n * slot_cap
        choices = tok_n * top_n
        f32, bf16 = jnp.float32, jnp.bfloat16
        h_both = jnp.stack([h_gate, h_up]).reshape(2, e_loc, rows_loc, fs_n, f_loc).transpose(3, 0, 1, 2, 4)
        h_all = lax.all_to_all(h_both, 'fsdp', 0, 0, tiled=True)
        x_split = x_disp.reshape(e_loc, rows_loc, fs_n, d_loc).transpose(2, 0, 1, 3)
        x_all = lax.all_to_all(x_split, 'fsdp', 0, 0, tiled=True)
        send_row = jnp.where(slot_pos >= 0, ((expert_idx // e_loc) * e_loc + expert_idx % e_loc) * slot_cap + slot_pos, slots_n).reshape(-1)
        src_choice = jnp.full((slots_n,), choices, jnp.int32).at[send_row].set(jnp.arange(choices, dtype=jnp.int32), mode='drop')
        send_dy = jnp.take(grad_out, src_choice // top_n, axis=0, mode='fill', fill_value=0).reshape(ep_n, e_loc * slot_cap, width)
        send_gate = jnp.take(gates.reshape(-1), src_choice, mode='fill', fill_value=0).reshape(ep_n, e_loc * slot_cap)
        recv_dy = lax.all_to_all(send_dy, 'ep', 0, 0, tiled=True).reshape(ep_n, e_loc, slot_cap, width).transpose(1, 0, 2, 3).reshape(e_loc, rows_loc, width)
        recv_gate = lax.all_to_all(send_gate, 'ep', 0, 0, tiled=True).reshape(ep_n, e_loc, slot_cap).transpose(1, 0, 2).reshape(e_loc, rows_loc)
        g_rows = (recv_dy.astype(f32) * recv_gate[..., None]).astype(bf16)
        dgate_rows = jnp.sum(recv_dy.astype(f32) * y_disp.astype(f32), axis=2)
        back_gate = lax.all_to_all(dgate_rows.reshape(e_loc, ep_n, slot_cap).transpose(1, 0, 2), 'ep', 0, 0, tiled=True).reshape(slots_n)
        g_all = lax.all_gather(g_rows, 'fsdp', axis=0)
        g_all = g_all.transpose(1, 0, 2, 3).reshape(e_loc, fs_n * rows_loc, width)
        d_act = jnp.einsum('erd,efd->erf', g_all, w_down, preferred_element_type=f32)
        h_rows = h_all.transpose(1, 2, 0, 3, 4).reshape(2, e_loc, fs_n * rows_loc, f_loc)
        gate_pre = h_rows[0].astype(f32)
        up_pre = h_rows[1].astype(f32)
        sig = jax.nn.sigmoid(gate_pre)
        silu = gate_pre * sig
        act = (silu * up_pre).astype(bf16)
        dh_gate = (d_act * up_pre * sig * (1.0 + gate_pre * (1.0 - sig))).astype(bf16)
        dh_up = (d_act * silu).astype(bf16)
        grad_w_down = jnp.einsum('erf,erd->efd', act, g_all, preferred_element_type=f32)
        dh_all = lax.all_gather(jnp.stack([dh_gate, dh_up]), 'fsdp', axis=0)
        x_rows = x_all.transpose(1, 0, 2, 3).reshape(e_loc, fs_n * rows_loc, d_loc)
        dh_g = dh_all[:, 0]
        dh_u = dh_all[:, 1]
        grad_w_gate = jnp.einsum('erd,serf->edsf', x_rows, dh_g, preferred_element_type=f32).reshape(e_loc, d_loc, hidden)
        grad_w_up = jnp.einsum('erd,serf->edsf', x_rows, dh_u, preferred_element_type=f32).reshape(e_loc, d_loc, hidden)
        wg = w_gate.reshape(e_loc, d_loc, fs_n, f_loc)
        wu = w_up.reshape(e_loc, d_loc, fs_n, f_loc)
        dx = (jnp.einsum('serf,edsf->erd', dh_g, wg, preferred_element_type=f32) + jnp.einsum('serf,edsf->erd', dh_u, wu, preferred_element_type=f32)).astype(bf16)
        dx_send = dx.reshape(e_loc, fs_n * ep_n, slot_cap, d_loc).transpose(1, 0, 2, 3)
        dx_back = lax.all_to_all(dx_send, ('fsdp', 'ep'), 0, 0, tiled=True)
        dx_back = dx_back.reshape(fs_n, slots_n, d_loc).transpose(1, 0, 2).reshape(slots_n, width)
        picked = jnp.take(dx_back, send_row, axis=0, mode='fill', fill_value=0).reshape(tok_n, top_n, width)
        grad_x = jnp.sum(picked.astype(f32), axis=1).astype(bf16)
        grad_gates = jnp.take(back_gate, send_row, mode='fill', fill_value=0).reshape(tok_n, top_n)
        return grad_x, grad_gates, grad_w_gate, grad_w_down, grad_w_up

    return jax.shard_map(local_backward, mesh=mesh, in_specs=(tok_spec, tok_spec, tok_spec, tok_spec, row_spec, row_spec, row_spec, row_spec, row_spec, row_spec, row_spec), out_specs=(tok_spec, tok_spec, row_spec, row_spec, row_spec), check_vma=False)
```

```python
import functools

import jax
import jax.numpy as jnp
from jax import lax
from jax.experimental import pallas as pl
from jax.experimental.pallas import tpu as pltpu
from jax.sharding import PartitionSpec as P

MESH = pl.DeviceIdType.MESH
F32, BF16 = jnp.float32, jnp.bfloat16
ANY = pl.BlockSpec(memory_space=pl.ANY)
VMEM = pl.BlockSpec(memory_space=pltpu.VMEM)


def remote(src, dst, send, recv, device):
    return pltpu.make_async_remote_copy(src_ref=src, dst_ref=dst, send_sem=send, recv_sem=recv, device_id=device, device_id_type=MESH)


def exchange_kernel(fs_n, ep_n, hg, hu, xs, dy_s, gt_s, y, h_all, x_all, g_all, dg_back, dy_r, gt_r, g_own, dg_own, h_ss, h_rs, x_ss, x_rs, d_ss, d_rs, t_ss, t_rs, g_ss, g_rs, b_ss, b_rs, l_sem):
    q = lax.axis_index('fsdp')
    p = lax.axis_index('ep')
    f_loc = h_all.shape[-1]
    barrier = pltpu.get_barrier_semaphore()
    zs = [lax.rem(q + k, fs_n) for k in range(1, fs_n)]
    es = [lax.rem(p + k, ep_n) for k in range(1, ep_n)]
    for z in zs:
        pl.semaphore_signal(barrier, inc=1, device_id={'fsdp': z}, device_id_type=MESH)
    for e in es:
        pl.semaphore_signal(barrier, inc=1, device_id={'ep': e}, device_id_type=MESH)
    pl.semaphore_wait(barrier, fs_n + ep_n - 2)
    d_copies = []
    for k, e in enumerate(es):
        d_copies.append(remote(dy_s.at[e], dy_r.at[:, p], d_ss.at[k], d_rs.at[k], {'ep': e}))
        d_copies.append(remote(gt_s.at[e], gt_r.at[:, p], t_ss.at[k], t_rs.at[k], {'ep': e}))
    for c in d_copies:
        c.start()
    l_d = pltpu.make_async_copy(dy_s.at[p], dy_r.at[:, p], l_sem.at[0])
    l_t = pltpu.make_async_copy(gt_s.at[p], gt_r.at[:, p], l_sem.at[1])
    l_d.start()
    l_t.start()
    h_copies = []
    for k, z in enumerate(zs):
        cols = pl.ds(pl.multiple_of(z * f_loc, 128), f_loc)
        h_copies.append(remote(hg.at[:, :, cols], h_all.at[0, :, q], h_ss.at[0, k], h_rs.at[0, k], {'fsdp': z}))
        h_copies.append(remote(hu.at[:, :, cols], h_all.at[1, :, q], h_ss.at[1, k], h_rs.at[1, k], {'fsdp': z}))
        h_copies.append(remote(xs.at[z], x_all.at[:, q], x_ss.at[k], x_rs.at[k], {'fsdp': z}))
    for c in h_copies:
        c.start()
    cols = pl.ds(pl.multiple_of(q * f_loc, 128), f_loc)
    locals_ = [
        pltpu.make_async_copy(hg.at[:, :, cols], h_all.at[0, :, q], l_sem.at[2]),
        pltpu.make_async_copy(hu.at[:, :, cols], h_all.at[1, :, q], l_sem.at[3]),
        pltpu.make_async_copy(xs.at[q], x_all.at[:, q], l_sem.at[4]),
    ]
    for c in locals_:
        c.start()
    l_d.wait()
    l_t.wait()
    for c in d_copies:
        c.wait()
    e_loc, _, cap, width = dy_r.shape

    def body(i, carry):
        e = i // ep_n
        s = i % ep_n
        gate = gt_r[e, s]
        acc = jnp.zeros((cap, 128), F32)
        for k in range(width // 128):
            sl = slice(k * 128, (k + 1) * 128)
            dy = dy_r[e, s, :, sl].astype(F32)
            g_own[e, s, :, sl] = (dy * gate).astype(BF16)
            acc = acc + dy * y[e, s, :, sl].astype(F32)
        dg_own[s, e] = jnp.broadcast_to(jnp.sum(acc, axis=1, keepdims=True), (cap, 128))
        return carry

    lax.fori_loop(0, e_loc * ep_n, body, 0)
    g_copies = []
    for k, z in enumerate(zs):
        g_copies.append(remote(g_own, g_all.at[:, q], g_ss.at[k], g_rs.at[k], {'fsdp': z}))
    for k, e in enumerate(es):
        g_copies.append(remote(dg_own.at[e], dg_back.at[p], b_ss.at[k], b_rs.at[k], {'ep': e}))
    for c in g_copies:
        c.start()
    l_g = pltpu.make_async_copy(g_own, g_all.at[:, q], l_sem.at[5])
    l_b = pltpu.make_async_copy(dg_own.at[p], dg_back.at[p], l_sem.at[6])
    l_g.start()
    l_b.start()
    for c in locals_:
        c.wait()
    l_g.wait()
    l_b.wait()
    for c in h_copies:
        c.wait()
    for c in g_copies:
        c.wait()


def gather_kernel(fs_n, dh, dh_all, s1, r1, s2, r2, l_sem):
    q = lax.axis_index('fsdp')
    right = lax.rem(q + 1, fs_n)
    left = lax.rem(q + fs_n - 1, fs_n)
    e_loc = dh.shape[1]
    barrier = pltpu.get_barrier_semaphore()
    for z in (left, right):
        pl.semaphore_signal(barrier, inc=1, device_id={'fsdp': z}, device_id_type=MESH)
    pl.semaphore_wait(barrier, 2)
    to_right, to_left = {}, {}
    for t in range(2):
        for e in range(e_loc):
            u = 1 - t
            to_right[t, e] = remote(dh.at[t, e], dh_all.at[q, t, e], s1.at[0, t, e], r1.at[0, t, e], {'fsdp': right})
            to_right[t, e].start()
            to_left[u, e] = remote(dh.at[u, e], dh_all.at[q, u, e], s1.at[1, u, e], r1.at[1, u, e], {'fsdp': left})
            to_left[u, e].start()
    own = pltpu.make_async_copy(dh, dh_all.at[q], l_sem)
    own.start()
    fwd = []
    for e in range(e_loc):
        to_right[0, e].wait_recv()
        c = remote(dh_all.at[left, 0, e], dh_all.at[left, 0, e], s2.at[0, e], r2.at[0, e], {'fsdp': right})
        c.start()
        fwd.append(c)
        to_left[1, e].wait_recv()
        c = remote(dh_all.at[right, 1, e], dh_all.at[right, 1, e], s2.at[1, e], r2.at[1, e], {'fsdp': left})
        c.start()
        fwd.append(c)
    own.wait()
    for e in range(e_loc):
        to_right[1, e].wait_recv()
        to_left[0, e].wait_recv()
    for e in range(e_loc):
        for t in range(2):
            to_right[t, e].wait_send()
            to_left[t, e].wait_send()
    for c in fwd:
        c.wait()


def hidden_kernel(g, h, w, dh, act):
    d_act = lax.dot_general(g[0], w[0], (((1,), (1,)), ((), ())), preferred_element_type=F32)
    gate_pre = h[0, 0].astype(F32)
    up_pre = h[1, 0].astype(F32)
    sig = jax.nn.sigmoid(gate_pre)
    silu = gate_pre * sig
    act[0] = (silu * up_pre).astype(BF16)
    dh[0, 0] = (d_act * up_pre * sig * (1.0 + gate_pre * (1.0 - sig))).astype(BF16)
    dh[1, 0] = (d_act * silu).astype(BF16)


def dx_kernel(dh, wg, wu, dx, acc):
    s = pl.program_id(1)
    nt = (((1,), (1,)), ((), ()))
    term = lax.dot_general(dh[0, 0, 0], wg[0], nt, preferred_element_type=F32) + lax.dot_general(dh[0, 1, 0], wu[0], nt, preferred_element_type=F32)

    @pl.when(s == 0)
    def _():
        acc[...] = term

    @pl.when(s > 0)
    def _():
        acc[...] += term

    @pl.when(s == pl.num_programs(1) - 1)
    def _():
        dx[0] = acc[...].astype(BF16)


def dw_kernel(x, dh, act, g, dwg, dwu, dwd):
    tn = (((0,), (0,)), ((), ()))
    dwg[0] = lax.dot_general(x[0], dh[0, 0, 0], tn, preferred_element_type=F32)
    dwu[0] = lax.dot_general(x[0], dh[0, 1, 0], tn, preferred_element_type=F32)
    dwd[0] = lax.dot_general(act[0], g[0], tn, preferred_element_type=F32)


def solution(mesh):
    ep_n = mesh.shape['ep']
    fs_n = mesh.shape['fsdp']
    tok_spec = P(('fsdp', 'ep'), None)
    row_spec = P('ep', 'fsdp', None)

    def local_backward(grad_out, expert_idx, slot_pos, gates, x_disp, h_gate, h_up, y_disp, w_gate, w_down, w_up):
        tok_n, top_n = expert_idx.shape
        e_loc, rows_loc, width = x_disp.shape
        hidden = h_gate.shape[2]
        f_loc = hidden // fs_n
        d_loc = width // fs_n
        cap = rows_loc // ep_n
        slots_n = e_loc * ep_n * cap
        rows = fs_n * rows_loc
        dma = pltpu.SemaphoreType.DMA
        x_split = x_disp.reshape(e_loc, rows_loc, fs_n, d_loc).transpose(2, 0, 1, 3)
        dest = jnp.where(slot_pos >= 0, expert_idx * cap + slot_pos, slots_n)
        hit = dest[None, :, :] == lax.broadcasted_iota(jnp.int32, (slots_n, tok_n, top_n), 0)
        pick = jnp.sum(hit, axis=2).astype(BF16)
        send_dy = jnp.dot(pick, grad_out, preferred_element_type=F32).astype(BF16).reshape(ep_n, e_loc, cap, width)
        send_gate = jnp.sum(jnp.where(hit, gates[None], 0.0), axis=(1, 2))
        send_gate = jnp.broadcast_to(send_gate[:, None], (slots_n, 128)).reshape(ep_n, e_loc, cap, 128)
        h_all, x_all, g_all, dg_back = pl.pallas_call(
            functools.partial(exchange_kernel, fs_n, ep_n),
            out_shape=(
                jax.ShapeDtypeStruct((2, e_loc, fs_n, rows_loc, f_loc), BF16),
                jax.ShapeDtypeStruct((e_loc, fs_n, rows_loc, d_loc), BF16),
                jax.ShapeDtypeStruct((e_loc, fs_n, ep_n, cap, width), BF16),
                jax.ShapeDtypeStruct((ep_n, e_loc, cap, 128), F32),
            ),
            in_specs=[ANY, ANY, ANY, VMEM, VMEM, VMEM],
            out_specs=[ANY, ANY, ANY, VMEM],
            scratch_shapes=[
                pltpu.VMEM((e_loc, ep_n, cap, width), BF16),
                pltpu.VMEM((e_loc, ep_n, cap, 128), F32),
                pltpu.VMEM((e_loc, ep_n, cap, width), BF16),
                pltpu.VMEM((ep_n, e_loc, cap, 128), F32),
                dma((2, fs_n - 1)), dma((2, fs_n - 1)), dma((fs_n - 1,)), dma((fs_n - 1,)),
                dma((ep_n - 1,)), dma((ep_n - 1,)), dma((ep_n - 1,)), dma((ep_n - 1,)),
                dma((fs_n - 1,)), dma((fs_n - 1,)), dma((ep_n - 1,)), dma((ep_n - 1,)),
                dma((7,)),
            ],
            compiler_params=pltpu.CompilerParams(collective_id=0, has_side_effects=True),
            name='exchange',
        )(h_gate, h_up, x_split, send_dy, send_gate, y_disp.reshape(e_loc, ep_n, cap, width))
        g_rows = g_all.reshape(e_loc, rows, width)
        h_rows = h_all.reshape(2, e_loc, rows, f_loc)
        x_rows = x_all.reshape(e_loc, rows, d_loc)
        dh, act = pl.pallas_call(
            hidden_kernel,
            grid=(e_loc,),
            out_shape=(jax.ShapeDtypeStruct((2, e_loc, rows, f_loc), BF16), jax.ShapeDtypeStruct((e_loc, rows, f_loc), BF16)),
            in_specs=[
                pl.BlockSpec((1, rows, width), lambda e: (e, 0, 0)),
                pl.BlockSpec((2, 1, rows, f_loc), lambda e: (0, e, 0, 0)),
                pl.BlockSpec((1, f_loc, width), lambda e: (e, 0, 0)),
            ],
            out_specs=[
                pl.BlockSpec((2, 1, rows, f_loc), lambda e: (0, e, 0, 0)),
                pl.BlockSpec((1, rows, f_loc), lambda e: (e, 0, 0)),
            ],
            name='hidden',
        )(g_rows, h_rows, w_down)
        dh_all = pl.pallas_call(
            functools.partial(gather_kernel, fs_n),
            out_shape=jax.ShapeDtypeStruct((fs_n, 2, e_loc, rows, f_loc), BF16),
            in_specs=[ANY],
            out_specs=ANY,
            scratch_shapes=[dma((2, 2, e_loc)), dma((2, 2, e_loc)), dma((2, e_loc)), dma((2, e_loc)), dma],
            compiler_params=pltpu.CompilerParams(collective_id=1, has_side_effects=True),
            name='gather',
        )(dh)
        dh_spec = pl.BlockSpec((1, 2, 1, rows, f_loc), lambda e, s: (s, 0, e, 0, 0))
        w_spec = pl.BlockSpec((1, d_loc, f_loc), lambda e, s: (e, 0, s))
        dx = pl.pallas_call(
            dx_kernel,
            grid=(e_loc, fs_n),
            out_shape=jax.ShapeDtypeStruct((e_loc, rows, d_loc), BF16),
            in_specs=[dh_spec, w_spec, w_spec],
            out_specs=pl.BlockSpec((1, rows, d_loc), lambda e, s: (e, 0, 0)),
            scratch_shapes=[pltpu.VMEM((rows, d_loc), F32)],
            name='dx',
        )(dh_all, w_gate, w_up)
        dx_send = dx.reshape(e_loc, fs_n * ep_n, cap, d_loc).transpose(1, 0, 2, 3)
        dx_back = lax.all_to_all(dx_send, ('fsdp', 'ep'), 0, 0, tiled=True)
        piece = slots_n // fs_n
        rows_spec = pl.BlockSpec((1, rows, f_loc // fs_n), lambda e, s: (e, 0, s))
        grad_w_gate, grad_w_up, grad_w_down = pl.pallas_call(
            dw_kernel,
            grid=(e_loc, fs_n),
            out_shape=(
                jax.ShapeDtypeStruct((e_loc, d_loc, hidden), F32),
                jax.ShapeDtypeStruct((e_loc, d_loc, hidden), F32),
                jax.ShapeDtypeStruct((e_loc, f_loc, width), F32),
            ),
            in_specs=[
                pl.BlockSpec((1, rows, d_loc), lambda e, s: (e, 0, 0)),
                dh_spec,
                pl.BlockSpec((1, rows, f_loc), lambda e, s: (e, 0, 0)),
                pl.BlockSpec((1, rows, width // 3), lambda e, s: (e, 0, jnp.minimum(s, 2))),
            ],
            out_specs=[w_spec, w_spec, pl.BlockSpec((1, f_loc, width // 3), lambda e, s: (e, 0, jnp.minimum(s, 2)))],
            cost_estimate=pl.CostEstimate(flops=2 * e_loc * rows * hidden * width, bytes_accessed=50_000_000, transcendentals=0),
            name='dw',
        )(x_rows, dh_all, act, g_rows)
        back = dx_back.reshape(fs_n, slots_n, d_loc).transpose(1, 0, 2).reshape(slots_n, width)
        picked = lax.dot_general(pick, back, (((0,), (0,)), ((), ())), preferred_element_type=F32)
        grad_x = picked.astype(BF16)
        grad_gates = jnp.sum(jnp.where(hit, dg_back.reshape(slots_n, 128)[:, 0][:, None, None], 0.0), axis=0)
        return grad_x, grad_gates, grad_w_gate, grad_w_down, grad_w_up

    return jax.shard_map(local_backward, mesh=mesh, in_specs=(tok_spec, tok_spec, tok_spec, tok_spec, row_spec, row_spec, row_spec, row_spec, row_spec, row_spec, row_spec), out_specs=(tok_spec, tok_spec, row_spec, row_spec, row_spec), check_vma=False)
```

```python
import functools

import jax
import jax.numpy as jnp
from jax import lax
from jax.experimental import pallas as pl
from jax.experimental.pallas import tpu as pltpu
from jax.sharding import PartitionSpec as P

MESH = pl.DeviceIdType.MESH
F32, BF16 = jnp.float32, jnp.bfloat16
ANY = pl.BlockSpec(memory_space=pl.ANY)
VMEM = pl.BlockSpec(memory_space=pltpu.VMEM)
ROOMS = (224, 256, 288, 352, 512)
BIG = 60 * 1024 * 1024


def remote(src, dst, send, recv, device):
    return pltpu.make_async_remote_copy(src_ref=src, dst_ref=dst, send_sem=send, recv_sem=recv, device_id=device, device_id_type=MESH)


def nn(a, b):
    return jnp.dot(a, b, preferred_element_type=F32)


def nt(a, b):
    return lax.dot_general(a, b, (((1,), (1,)), ((), ())), preferred_element_type=F32)


def tn(a, b):
    return lax.dot_general(a, b, (((0,), (0,)), ((), ())), preferred_element_type=F32)


def packer(spot, room):
    return jnp.where(lax.broadcasted_iota(jnp.int32, (room, spot.shape[1]), 0) == spot, 1.0, 0.0).astype(BF16)


def counts_kernel(fs_n, ep_n, mine, table, e_ss, e_rs, z_ss, z_rs, l_sem):
    q = lax.axis_index('fsdp')
    p = lax.axis_index('ep')
    barrier = pltpu.get_barrier_semaphore()
    zs = [lax.rem(q + k, fs_n) for k in range(1, fs_n)]
    es = [lax.rem(p + k, ep_n) for k in range(1, ep_n)]
    for z in zs:
        pl.semaphore_signal(barrier, inc=1, device_id={'fsdp': z}, device_id_type=MESH)
    for e in es:
        pl.semaphore_signal(barrier, inc=1, device_id={'ep': e}, device_id_type=MESH)
    pl.semaphore_wait(barrier, fs_n + ep_n - 2)
    copies = [remote(mine, table.at[q, p], e_ss.at[k], e_rs.at[k], {'ep': e}) for k, e in enumerate(es)]
    for c in copies:
        c.start()
    own = pltpu.make_async_copy(mine, table.at[q, p], l_sem)
    own.start()
    own.wait()
    for c in copies:
        c.wait()
    copies = [remote(table.at[q], table.at[q], z_ss.at[k], z_rs.at[k], {'fsdp': z}) for k, z in enumerate(zs)]
    for c in copies:
        c.start()
    for c in copies:
        c.wait()


def exchange_kernel(fs_n, ep_n, hg, hu, x, spot, dy_s, gt_s, y, h_all, x_all, g_all, dg_back, dy_r, gt_r, g_own, dg_own, hc, xc, h_in, x_in, gc, g_in, h_half, x_half, g_half, w_ss, w_rs, d_ss, d_rs, t_ss, t_rs, b_ss, b_rs, z_ss, z_rs, f_ss, f_rs, l_sem):
    q = lax.axis_index('fsdp')
    p = lax.axis_index('ep')
    j = lax.rem(p, 2)
    pair = {'ep': p + 1 - 2 * j}
    half = x_in.shape[1]
    f_loc = h_all.shape[-1]
    keep = pl.ds(pl.multiple_of(j * half, 16), half)
    give = pl.ds(pl.multiple_of((1 - j) * half, 16), half)
    barrier = pltpu.get_barrier_semaphore()
    zs = [lax.rem(q + k, fs_n) for k in range(1, fs_n)]
    es = [lax.rem(p + k, ep_n) for k in range(1, ep_n)]
    for z in zs:
        pl.semaphore_signal(barrier, inc=1, device_id={'fsdp': z}, device_id_type=MESH)
    for e in es:
        pl.semaphore_signal(barrier, inc=1, device_id={'ep': e}, device_id_type=MESH)
    pl.semaphore_wait(barrier, fs_n + ep_n - 2)
    d_copies = []
    for k, e in enumerate(es):
        d_copies.append(remote(dy_s.at[e], dy_r.at[:, p], d_ss.at[k], d_rs.at[k], {'ep': e}))
        d_copies.append(remote(gt_s.at[e], gt_r.at[:, p], t_ss.at[k], t_rs.at[k], {'ep': e}))
    for c in d_copies:
        c.start()
    l_d = pltpu.make_async_copy(dy_s.at[p], dy_r.at[:, p], l_sem.at[0])
    l_t = pltpu.make_async_copy(gt_s.at[p], gt_r.at[:, p], l_sem.at[1])
    l_d.start()
    l_t.start()
    pack = packer(spot[pl.ds(q, 1)], gc.shape[0])
    flat = pack.shape[1]
    d_loc = xc.shape[2]

    def pack_cols(z, carry):
        cols = pl.ds(pl.multiple_of(z * f_loc, 128), f_loc)
        for t, h in enumerate((hg, hu)):
            hc[t, :, cols] = nn(pack, h[:, :, cols].reshape(flat, f_loc)).astype(BF16)
        return carry

    lax.fori_loop(0, fs_n, pack_cols, 0)
    packed_x = nn(pack, x[...].reshape(flat, x.shape[2])).astype(BF16)
    for z in range(fs_n):
        xc[z] = packed_x[:, z * d_loc:(z + 1) * d_loc]
    swap_h = remote(hc.at[:, give], h_in, w_ss.at[0], w_rs.at[0], pair)
    swap_x = remote(xc.at[:, give], x_in, w_ss.at[1], w_rs.at[1], pair)
    swap_h.start()
    swap_x.start()
    swap_h.wait()
    swap_x.wait()

    def add_cols(z, carry):
        cols = pl.ds(pl.multiple_of(z * f_loc, 128), f_loc)
        for t in range(2):
            h_half[z, t] = hc[t, keep, cols] + h_in[t, :, cols]
        return carry

    lax.fori_loop(0, fs_n, add_cols, 0)
    for z in range(fs_n):
        x_half[z] = xc[z, keep] + x_in[z]
    sends = []
    for k, z in enumerate(zs):
        sends.append(remote(h_half.at[z], h_all.at[q, :, keep], z_ss.at[0, k], z_rs.at[0, k], {'fsdp': z}))
        sends.append(remote(x_half.at[z], x_all.at[q, keep], z_ss.at[1, k], z_rs.at[1, k], {'fsdp': z}))
    for c in sends:
        c.start()
    own = [
        pltpu.make_async_copy(h_half.at[q], h_all.at[q, :, keep], l_sem.at[2]),
        pltpu.make_async_copy(x_half.at[q], x_all.at[q, keep], l_sem.at[3]),
        remote(h_half.at[q], h_all.at[q, :, keep], f_ss.at[0, fs_n - 1], f_rs.at[0, fs_n - 1], pair),
        remote(x_half.at[q], x_all.at[q, keep], f_ss.at[1, fs_n - 1], f_rs.at[1, fs_n - 1], pair),
    ]
    for c in own:
        c.start()
    l_d.wait()
    l_t.wait()
    for c in d_copies:
        c.wait()
    e_loc, _, cap, width = dy_r.shape

    def body(i, carry):
        e = i // ep_n
        s = i % ep_n
        gate = gt_r[e, s]
        acc = jnp.zeros((cap, 128), F32)
        for k in range(width // 128):
            sl = slice(k * 128, (k + 1) * 128)
            dy = dy_r[e, s, :, sl].astype(F32)
            g_own[e, s, :, sl] = (dy * gate).astype(BF16)
            acc = acc + dy * y[e, s, :, sl].astype(F32)
        dg_own[s, e] = jnp.broadcast_to(jnp.sum(acc, axis=1, keepdims=True), (cap, 128))
        return carry

    lax.fori_loop(0, e_loc * ep_n, body, 0)
    gc[...] = nn(pack, g_own[...].reshape(flat, width)).astype(BF16)
    swap_g = remote(gc.at[give], g_in, w_ss.at[2], w_rs.at[2], pair)
    swap_g.start()
    back = []
    for k, e in enumerate(es):
        back.append(remote(dg_own.at[e], dg_back.at[p], b_ss.at[k], b_rs.at[k], {'ep': e}))
    for c in back:
        c.start()
    l_b = pltpu.make_async_copy(dg_own.at[p], dg_back.at[p], l_sem.at[4])
    l_b.start()
    swap_g.wait()
    g_half[...] = gc[keep] + g_in[...]
    g_sends = [remote(g_half, g_all.at[q, keep], z_ss.at[2, k], z_rs.at[2, k], {'fsdp': z}) for k, z in enumerate(zs)]
    g_own_copies = [
        pltpu.make_async_copy(g_half, g_all.at[q, keep], l_sem.at[5]),
        remote(g_half, g_all.at[q, keep], f_ss.at[2, fs_n - 1], f_rs.at[2, fs_n - 1], pair),
    ]
    for c in g_sends + g_own_copies:
        c.start()
    fwd = []
    for k in range(fs_n - 1):
        src = lax.rem(q + fs_n - k - 1, fs_n)
        for a, (ref, c) in enumerate(((h_all.at[src, :, keep], sends[2 * k]), (x_all.at[src, keep], sends[2 * k + 1]), (g_all.at[src, keep], g_sends[k]))):
            c.wait_recv()
            f = remote(ref, ref, f_ss.at[a, k], f_rs.at[a, k], pair)
            f.start()
            fwd.append(f)
    for c in own + g_own_copies + fwd + back:
        c.wait()
    l_b.wait()
    for c in sends + g_sends:
        c.wait_send()


def gather_kernel(fs_n, dhc, dh_all, d_in, d_half, w_ss, w_rs, r_ss, r_rs, s_ss, s_rs, f_ss, f_rs, l_sem):
    q = lax.axis_index('fsdp')
    p = lax.axis_index('ep')
    j = lax.rem(p, 2)
    pair = {'ep': p + 1 - 2 * j}
    half = d_half.shape[2]
    chunks = d_half.shape[0]
    keep = pl.ds(pl.multiple_of(j * half, 16), half)
    give = pl.ds(pl.multiple_of((1 - j) * half, 16), half)
    has_right, has_left = q < fs_n - 1, q > 0
    right = {'fsdp': jnp.minimum(q + 1, fs_n - 1)}
    left = {'fsdp': jnp.maximum(q - 1, 0)}
    barrier = pltpu.get_barrier_semaphore()
    pl.semaphore_signal(barrier, inc=1, device_id=pair, device_id_type=MESH)

    @pl.when(has_right)
    def _():
        pl.semaphore_signal(barrier, inc=1, device_id=right, device_id_type=MESH)

    @pl.when(has_left)
    def _():
        pl.semaphore_signal(barrier, inc=1, device_id=left, device_id_type=MESH)

    pl.semaphore_wait(barrier, 1 + has_right.astype(jnp.int32) + has_left.astype(jnp.int32))
    swaps = [remote(dhc.at[c, :, give], d_in.at[c], w_ss.at[c], w_rs.at[c], pair) for c in range(chunks)]
    for c in swaps:
        c.start()

    def place(s, c):
        return dh_all.at[s, c, :, keep]

    def to_right(k, c):
        s = jnp.maximum(q - k, 0)
        return remote(d_half.at[c] if k == 0 else place(s, c), place(s, c), r_ss.at[k, c], r_rs.at[k, c], right)

    def to_left(k, c):
        s = jnp.minimum(q + k, fs_n - 1)
        return remote(d_half.at[c] if k == 0 else place(s, c), place(s, c), s_ss.at[k, c], s_rs.at[k, c], left)

    def from_left(k, c):
        s = jnp.maximum(q - k, 0)
        return remote(place(s, c), place(s, c), r_ss.at[k - 1, c], r_rs.at[k - 1, c], right)

    def from_right(k, c):
        s = jnp.minimum(q + k, fs_n - 1)
        return remote(place(s, c), place(s, c), s_ss.at[k - 1, c], s_rs.at[k - 1, c], left)

    own = []
    for c in range(chunks):
        swaps[c].wait()
        d_half[c] = dhc[c, :, keep] + d_in[c]
        o = [pltpu.make_async_copy(d_half.at[c], place(q, c), l_sem.at[c]), remote(d_half.at[c], place(q, c), f_ss.at[0, c], f_rs.at[0, c], pair)]
        own += o

        @pl.when(has_right)
        def _(c=c):
            to_right(0, c).start()

        @pl.when(has_left)
        def _(c=c):
            to_left(0, c).start()

        for x in o:
            x.start()

    def pass_on(s, c, slot):
        return remote(place(s, c), place(s, c), f_ss.at[slot, c], f_rs.at[slot, c], pair)

    for k in range(1, fs_n):
        for c in range(chunks):
            @pl.when(q - k >= 0)
            def _(k=k, c=c):
                from_left(k, c).wait_recv()
                pass_on(jnp.maximum(q - k, 0), c, k).start()

                @pl.when(has_right)
                def _():
                    to_right(k, c).start()

            @pl.when(q + k < fs_n)
            def _(k=k, c=c):
                from_right(k, c).wait_recv()
                pass_on(jnp.minimum(q + k, fs_n - 1), c, fs_n - 1 + k).start()

                @pl.when(has_left)
                def _():
                    to_left(k, c).start()

    for x in own:
        x.wait()
    for k in range(fs_n):
        for c in range(chunks):
            @pl.when((q - k >= 0) & has_right)
            def _(k=k, c=c):
                to_right(k, c).wait_send()

            @pl.when((q + k < fs_n) & has_left)
            def _(k=k, c=c):
                to_left(k, c).wait_send()

            if k > 0:
                @pl.when(q - k >= 0)
                def _(k=k, c=c):
                    pass_on(jnp.maximum(q - k, 0), c, k).wait()

                @pl.when(q + k < fs_n)
                def _(k=k, c=c):
                    pass_on(jnp.minimum(q + k, fs_n - 1), c, fs_n - 1 + k).wait()


def hidden_kernel(h_all, x_all, g_all, spot, w, dhc, act, g_rows, x_rows, hs, ds):
    fs_n, room = spot.shape[0], dhc.shape[2]
    e_loc, rows, f_loc = act.shape
    part = rows // fs_n

    def unpack(i, carry):
        m = packer(spot[pl.ds(i, 1)], room)
        at = pl.ds(pl.multiple_of(i * part, 16), part)
        for t in range(2):
            hs[t, :, at] = tn(m, h_all[i, t]).astype(BF16).reshape(e_loc, part, f_loc)
        g_rows[:, at] = tn(m, g_all[i]).astype(BF16).reshape(e_loc, part, g_rows.shape[2])
        x_rows[:, at] = tn(m, x_all[i]).astype(BF16).reshape(e_loc, part, x_rows.shape[2])
        return carry

    lax.fori_loop(0, fs_n, unpack, 0)

    def expert(e, carry):
        d_act = nt(g_rows[e], w[e])
        gate_pre = hs[0, e].astype(F32)
        up_pre = hs[1, e].astype(F32)
        sig = jax.nn.sigmoid(gate_pre)
        silu = gate_pre * sig
        act[e] = (silu * up_pre).astype(BF16)
        ds[0, e] = (d_act * up_pre * sig * (1.0 + gate_pre * (1.0 - sig))).astype(BF16)
        ds[1, e] = (d_act * silu).astype(BF16)
        return carry

    lax.fori_loop(0, e_loc, expert, 0)

    def pack(i, carry):
        at = pl.ds(pl.multiple_of(i * part, 16), part)
        m = packer(spot[pl.ds(i, 1)], room)
        for t in range(2):
            dhc[i, t] = nn(m, ds[t, :, at].reshape(e_loc * part, f_loc)).astype(BF16)
        return carry

    lax.fori_loop(0, fs_n, pack, 0)


def dx_kernel(dh_all, spot, wg, wu, dh, dx, acc):
    s = pl.program_id(0)
    _, fs_n, _, room, f_loc = dh_all.shape
    _, _, e_loc, rows, _ = dh.shape
    part = rows // fs_n
    for i in range(fs_n):
        m = packer(spot[i:i + 1], room)
        for t in range(2):
            dh[0, t, :, i * part:(i + 1) * part] = tn(m, dh_all[0, i, t]).astype(BF16).reshape(e_loc, part, f_loc)

    @pl.when(s == 0)
    def _():
        acc[...] = jnp.zeros_like(acc)

    for e in range(e_loc):
        acc[e] += nt(dh[0, 0, e], wg[e]) + nt(dh[0, 1, e], wu[e])

    @pl.when(s == pl.num_programs(0) - 1)
    def _():
        dx[...] = acc[...].astype(BF16)


def dw_kernel(dh, x, act, g, dwg, dwu, dwd):
    for e in range(x.shape[0]):
        dwg[e] = tn(x[e], dh[0, 0, e])
        dwu[e] = tn(x[e], dh[0, 1, e])
    dwd[0] = tn(act[0], g[0])


def solution(mesh):
    ep_n = mesh.shape['ep']
    fs_n = mesh.shape['fsdp']
    tok_spec = P(('fsdp', 'ep'), None)
    row_spec = P('ep', 'fsdp', None)

    def local_backward(grad_out, expert_idx, slot_pos, gates, x_disp, h_gate, h_up, y_disp, w_gate, w_down, w_up):
        tok_n, top_n = expert_idx.shape
        e_loc, rows_loc, width = x_disp.shape
        hidden = h_gate.shape[2]
        f_loc = hidden // fs_n
        d_loc = width // fs_n
        cap = rows_loc // ep_n
        slots_n = e_loc * ep_n * cap
        rows = fs_n * rows_loc
        experts = e_loc * ep_n
        dma = pltpu.SemaphoreType.DMA
        dest = jnp.where(slot_pos >= 0, expert_idx * cap + slot_pos, slots_n)
        hit = dest[None, :, :] == lax.broadcasted_iota(jnp.int32, (slots_n, tok_n, top_n), 0)
        pick = jnp.sum(hit, axis=2).astype(BF16)
        filled = jnp.sum(hit, axis=(1, 2)).astype(jnp.int32)
        mine = jnp.broadcast_to(jnp.pad(jnp.sum(filled.reshape(1, experts, cap), axis=2), ((0, 0), (0, 128 - experts))), (8, 128))
        counts = pl.pallas_call(
            functools.partial(counts_kernel, fs_n, ep_n),
            out_shape=jax.ShapeDtypeStruct((fs_n, ep_n, 8, 128), jnp.int32),
            in_specs=[VMEM],
            out_specs=VMEM,
            scratch_shapes=[dma((ep_n - 1,)), dma((ep_n - 1,)), dma((fs_n - 1,)), dma((fs_n - 1,)), dma],
            compiler_params=pltpu.CompilerParams(collective_id=2 * len(ROOMS), has_side_effects=True),
            name='counts',
        )(mine)[:, :, 0, :experts]
        need = jnp.max(jnp.sum(counts.reshape(fs_n, ep_n, experts // (2 * e_loc), 2 * e_loc), axis=(1, 3)))
        p = lax.axis_index('ep')
        mine = lax.dynamic_slice_in_dim(counts, p * e_loc, e_loc, 2).transpose(0, 2, 1).reshape(fs_n, e_loc * ep_n)
        before = lax.broadcasted_iota(jnp.int32, (e_loc * ep_n, e_loc * ep_n), 0) < lax.broadcasted_iota(jnp.int32, (e_loc * ep_n, e_loc * ep_n), 1)
        start = jnp.sum(jnp.where(before[None], mine[:, :, None], 0), axis=1)
        slot = lax.broadcasted_iota(jnp.int32, (fs_n, e_loc * ep_n, cap), 2)
        rank = jnp.where(slot < mine[:, :, None], start[:, :, None] + slot, -1).reshape(fs_n, e_loc * rows_loc)
        send_dy = jnp.dot(pick, grad_out, preferred_element_type=F32).astype(BF16).reshape(ep_n, e_loc, cap, width)
        send_gate = jnp.sum(jnp.where(hit, gates[None], 0.0), axis=(1, 2))
        send_gate = jnp.broadcast_to(send_gate[:, None], (slots_n, 128)).reshape(ep_n, e_loc, cap, 128)

        w_spec = pl.BlockSpec((e_loc, d_loc, f_loc), lambda s: (0, 0, s))
        dh_spec = pl.BlockSpec((1, 2, e_loc, rows, f_loc), lambda s: (s, 0, 0, 0, 0))

        def packed(room, rank, send_dy, send_gate, x_disp, h_gate, h_up, y_disp, w_gate, w_down, w_up):
            half = room // 2
            p = lax.axis_index('ep')
            spot = jnp.where(rank < 0, -1, jnp.where(p % 2 == 0, rank, room - 1 - rank))
            h_all, x_all, g_all, dg_back = pl.pallas_call(
                functools.partial(exchange_kernel, fs_n, ep_n),
                out_shape=(
                    jax.ShapeDtypeStruct((fs_n, 2, room, f_loc), BF16),
                    jax.ShapeDtypeStruct((fs_n, room, d_loc), BF16),
                    jax.ShapeDtypeStruct((fs_n, room, width), BF16),
                    jax.ShapeDtypeStruct((ep_n, e_loc, cap, 128), F32),
                ),
                in_specs=[VMEM] * 7,
                out_specs=[ANY, ANY, ANY, VMEM],
                scratch_shapes=[
                    pltpu.VMEM((e_loc, ep_n, cap, width), BF16),
                    pltpu.VMEM((e_loc, ep_n, cap, 128), F32),
                    pltpu.VMEM((e_loc, ep_n, cap, width), BF16),
                    pltpu.VMEM((ep_n, e_loc, cap, 128), F32),
                    pltpu.VMEM((2, room, hidden), BF16),
                    pltpu.VMEM((fs_n, room, d_loc), BF16),
                    pltpu.VMEM((2, half, hidden), BF16),
                    pltpu.VMEM((fs_n, half, d_loc), BF16),
                    pltpu.VMEM((room, width), BF16),
                    pltpu.VMEM((half, width), BF16),
                    pltpu.VMEM((fs_n, 2, half, f_loc), BF16),
                    pltpu.VMEM((fs_n, half, d_loc), BF16),
                    pltpu.VMEM((half, width), BF16),
                    dma((3,)), dma((3,)),
                    dma((ep_n - 1,)), dma((ep_n - 1,)), dma((ep_n - 1,)), dma((ep_n - 1,)), dma((ep_n - 1,)), dma((ep_n - 1,)),
                    dma((3, fs_n - 1)), dma((3, fs_n - 1)), dma((3, fs_n)), dma((3, fs_n)),
                    dma((6,)),
                ],
                compiler_params=pltpu.CompilerParams(collective_id=2 * ROOMS.index(room), has_side_effects=True, vmem_limit_bytes=BIG),
                name='exchange',
            )(h_gate, h_up, x_disp, spot, send_dy, send_gate, y_disp.reshape(e_loc, ep_n, cap, width))
            dhc, act, g_rows, x_rows = pl.pallas_call(
                hidden_kernel,
                out_shape=(
                    jax.ShapeDtypeStruct((fs_n, 2, room, f_loc), BF16),
                    jax.ShapeDtypeStruct((e_loc, rows, f_loc), BF16),
                    jax.ShapeDtypeStruct((e_loc, rows, width), BF16),
                    jax.ShapeDtypeStruct((e_loc, rows, d_loc), BF16),
                ),
                in_specs=[VMEM] * 5,
                out_specs=[VMEM] * 4,
                scratch_shapes=[pltpu.VMEM((2, e_loc, rows, f_loc), BF16), pltpu.VMEM((2, e_loc, rows, f_loc), BF16)],
                compiler_params=pltpu.CompilerParams(vmem_limit_bytes=BIG),
                name='hidden',
            )(h_all, x_all, g_all, spot, w_down)
            dh_all = pl.pallas_call(
                functools.partial(gather_kernel, fs_n),
                out_shape=jax.ShapeDtypeStruct((fs_n, fs_n, 2, room, f_loc), BF16),
                in_specs=[VMEM],
                out_specs=ANY,
                scratch_shapes=[
                    pltpu.VMEM((fs_n, 2, half, f_loc), BF16),
                    pltpu.VMEM((fs_n, 2, half, f_loc), BF16),
                    dma((fs_n,)), dma((fs_n,)),
                    dma((fs_n, fs_n)), dma((fs_n, fs_n)), dma((fs_n, fs_n)), dma((fs_n, fs_n)),
                    dma((2 * fs_n - 1, fs_n)), dma((2 * fs_n - 1, fs_n)), dma((fs_n,)),
                ],
                compiler_params=pltpu.CompilerParams(collective_id=2 * ROOMS.index(room) + 1, has_side_effects=True, vmem_limit_bytes=BIG),
                name='gather',
            )(dhc)
            dh, dx = pl.pallas_call(
                dx_kernel,
                grid=(fs_n,),
                out_shape=(jax.ShapeDtypeStruct((fs_n, 2, e_loc, rows, f_loc), BF16), jax.ShapeDtypeStruct((e_loc, rows, d_loc), BF16)),
                in_specs=[pl.BlockSpec((1, fs_n, 2, room, f_loc), lambda s: (s, 0, 0, 0, 0)), pl.BlockSpec((fs_n, e_loc * rows_loc), lambda s: (0, 0)), w_spec, w_spec],
                out_specs=[dh_spec, pl.BlockSpec((e_loc, rows, d_loc), lambda s: (0, 0, 0))],
                scratch_shapes=[pltpu.VMEM((e_loc, rows, d_loc), F32)],
                compiler_params=pltpu.CompilerParams(vmem_limit_bytes=BIG),
                name='dx',
            )(dh_all, spot, w_gate, w_up)
            return dh, dx, act, g_rows, x_rows, dg_back

        which = jnp.sum((need > jnp.array(ROOMS[:-1])).astype(jnp.int32))
        dh, dx, act, g_rows, x_rows, dg_back = lax.switch(which, [functools.partial(packed, room) for room in ROOMS], rank, send_dy, send_gate, x_disp, h_gate, h_up, y_disp, w_gate, w_down, w_up)
        dx_send = dx.reshape(e_loc, fs_n * ep_n, cap, d_loc).transpose(1, 0, 2, 3)
        dx_back = lax.all_to_all(dx_send, ('fsdp', 'ep'), 0, 0, tiled=True)
        grad_w_gate, grad_w_up, grad_w_down = pl.pallas_call(
            dw_kernel,
            grid=(fs_n,),
            out_shape=(
                jax.ShapeDtypeStruct((e_loc, d_loc, hidden), F32),
                jax.ShapeDtypeStruct((e_loc, d_loc, hidden), F32),
                jax.ShapeDtypeStruct((e_loc, f_loc, width), F32),
            ),
            in_specs=[
                dh_spec,
                pl.BlockSpec((e_loc, rows, d_loc), lambda s: (0, 0, 0)),
                pl.BlockSpec((1, rows, f_loc), lambda s: (s, 0, 0)),
                pl.BlockSpec((1, rows, width), lambda s: (s, 0, 0)),
            ],
            out_specs=[w_spec, w_spec, pl.BlockSpec((1, f_loc, width), lambda s: (s, 0, 0))],
            compiler_params=pltpu.CompilerParams(vmem_limit_bytes=BIG),
            cost_estimate=pl.CostEstimate(flops=2 * e_loc * rows * hidden * width, bytes_accessed=50_000_000, transcendentals=0),
            name='dw',
        )(dh, x_rows, act, g_rows)
        back = dx_back.reshape(fs_n, slots_n, d_loc).transpose(1, 0, 2).reshape(slots_n, width)
        grad_x = tn(pick, back).astype(BF16)
        grad_gates = jnp.sum(jnp.where(hit, dg_back.reshape(slots_n, 128)[:, 0][:, None, None], 0.0), axis=0)
        return grad_x, grad_gates, grad_w_gate, grad_w_down, grad_w_up

    return jax.shard_map(local_backward, mesh=mesh, in_specs=(tok_spec, tok_spec, tok_spec, tok_spec, row_spec, row_spec, row_spec, row_spec, row_spec, row_spec, row_spec), out_specs=(tok_spec, tok_spec, row_spec, row_spec, row_spec), check_vma=False)
```
